32 devices in a mesh: img: 8 (over y, x, core), ori: 4 (over z).
Axes of the slice: x: 2, y: 2, z: 4, core: 2. Of those that a mesh axis runs over, the one named last changes fastest.
Arguments:
- images: bfloat16 [4096, 4096], P('img'), may hold values from -6 to 6
- ctf_class: int32 [4096], P('img'), may hold values from 0 to 15
- class_mask: int32 [4096, 8], P('img'), may hold values from 0 to 1, as said below
- precision: float32 [4096], P('img'), may hold values from 0.02 to 0.5
- class_log_prior: float32 [4096, 8], P('img'), may hold values from -6 to 406
- ctf_filters: float32 [16, 4096], replicated, may hold values from -1 to 1
- volume_coef: bfloat16 [8, 16, 2, 4096], P(None, 'img'), may hold values from -6 to 6
- slice_ops: bfloat16 [8, 4096, 64], replicated, may hold values from -0.09375 to 0.09375
- tilt_index: int32 [64], P('ori'), may hold values from 0 to 7
- azimuth_index: int32 [64], P('ori'), may hold values from 0 to 31
Outputs:
- coef_sum: float32 [8, 16, 2, 4096], P(None, 'img')
- log_evidence: float32 [4096], P('img')
- class_posterior: float32 [4096, 8], P('img')
The draws below stay inside these ranges and needn't reach their ends.
Inputs may be any that keep to these rules, and one draw needn't show every extreme that they name: `class_mask`: every image allows at least one class.
All inputs are finite; a program needn't handle non-finite values.
Results may differ from the reference program's by a relative error of at most 0.024.
The reference program's roundings to bfloat16 on the way count: a program that leaves them out, or rounds other values in their place, can miss the bound.
Values may be sent and summed in bfloat16 or wider, within the bound.
No kernel may reach another device: no remote copies, remote signals or barrier semaphores. Data moves between devices by JAX's collectives and lax.ppermute only.
A program may use at most 192 MiB of HBM per device.

```python
import math
import jax
import jax.numpy as jnp
from jax import lax

K = 8
R = 16
ORD = 64
ANG = 128
NTILT = 8
NAZI = 32
NCTF = 16
ORI_DEV = 16
LM = 4096
P_SIZE = 4096
IMAGES = 4096
ORIENT = 64
N_ORI = 4


def draw_class_mask(key, part):
    random_bits = jax.random.randint(jax.random.fold_in(key, 11), (IMAGES, K), 0, 2)
    picked = jax.random.randint(jax.random.fold_in(key, 12), (IMAGES,), 0, K)
    chosen = (picked[:, None] == jnp.arange(K)[None, :]).astype(jnp.int32)
    return jnp.maximum(random_bits, chosen).astype(jnp.int32)


def draw_class_log_prior(key, part):
    rough = jax.random.uniform(jax.random.fold_in(key, 21), (IMAGES, K), jnp.float32, -2.0, 2.0)
    lifted = jax.random.randint(jax.random.fold_in(key, 22), (IMAGES,), 0, 5) == 0
    shift = jax.random.uniform(jax.random.fold_in(key, 23), (IMAGES,), jnp.float32, 100.0, 400.0)
    rival = jax.random.randint(jax.random.fold_in(key, 24), (IMAGES,), 0, K)
    drop = jax.random.uniform(jax.random.fold_in(key, 25), (IMAGES,), jnp.float32, 1.0, 3.0)
    best = jnp.max(rough, axis=1)
    is_rival = rival[:, None] == jnp.arange(K)[None, :]
    paired = jnp.where(is_rival & lifted[:, None], (best - drop)[:, None], rough)
    lifted_rows = paired + jnp.where(lifted, shift, 0.0)[:, None]
    return lifted_rows.astype(jnp.float32)


def touch_ends(entries, own_key, least, top_value):
    longest = entries.shape.index(max(entries.shape))
    spots = []
    for shift in (0, 1):
        where = [jax.random.randint(jax.random.fold_in(own_key, axis), (), 0, length) for axis, length in enumerate(entries.shape)]
        where[longest] = (where[longest] + shift) % entries.shape[longest]
        spots.append(tuple(where))
    return entries.at[spots[0]].set(least).at[spots[1]].set(top_value)


def block_scale(stream_key, shape, shards, least, high):
    def one(dim, shards_of):
        steps = jax.random.uniform(jax.random.fold_in(jax.random.fold_in(stream_key, 6), dim), (shards_of,), jnp.float32, least / len(shards), high / len(shards))
        return jnp.repeat(jnp.exp(steps), shape[dim] // shards_of).reshape((-1,) + (1,) * (len(shape) - dim - 1))

    loudness = one(*shards[0])
    for cut in shards[1:]:
        loudness = loudness * one(*cut)
    return loudness


def gaussian(key, shape, width, limit, split=(), held_as=jnp.bfloat16):
    loudness = block_scale(key, shape, split, -0.22, 0.18) if split else 1.0
    drawn = jax.random.normal(key, shape, jnp.float32) * width * loudness
    return jnp.minimum(jnp.maximum(drawn, -limit), limit).astype(held_as)


def setup_inputs(seed: int = 0) -> dict:
    key_of = jax.random.split(jax.random.key(seed), 11)
    images = gaussian(key_of[0], (IMAGES, P_SIZE), 1.0, 6.0, ((0, 8),))
    ctf_class = touch_ends(jax.random.randint(key_of[1], (IMAGES,), 0, NCTF), jax.random.fold_in(key_of[1], 1), 0, NCTF - 1).astype(jnp.int32)
    class_mask = draw_class_mask(jax.random.fold_in(key_of[10], 71), 0)
    precision = jnp.clip(jnp.exp(math.log(0.5) - 3.218876 * jax.random.uniform(key_of[3], (IMAGES,), jnp.float32) ** block_scale(key_of[3], (IMAGES,), ((0, 8),), -0.2, 0.2)), 0.02, 0.5)
    class_log_prior = draw_class_log_prior(jax.random.fold_in(key_of[10], 71), 0)
    ctf_filters = jnp.clip(jax.random.uniform(key_of[5], (NCTF, P_SIZE), jnp.float32, -1.0, 1.0), -1.0, 1.0)
    volume_coef = gaussian(key_of[6], (K, R, 2, LM), 1.0, 6.0, ((1, 8),))
    slice_ops = gaussian(key_of[7], (NTILT, LM, ORD), LM ** -0.5, 0.09375)
    tilt_index = touch_ends(jax.random.randint(key_of[8], (ORIENT,), 0, NTILT), jax.random.fold_in(key_of[8], 1), 0, NTILT - 1).astype(jnp.int32)
    azimuth_index = touch_ends(jax.random.randint(key_of[9], (ORIENT,), 0, NAZI), jax.random.fold_in(key_of[9], 1), 0, NAZI - 1).astype(jnp.int32)
    return dict(images=images, ctf_class=ctf_class, class_mask=class_mask, precision=precision, class_log_prior=class_log_prior, ctf_filters=ctf_filters, volume_coef=volume_coef, slice_ops=slice_ops, tilt_index=tilt_index, azimuth_index=azimuth_index)


def synth_table():
    orders = (jnp.arange(ORD) - ORD // 2).astype(jnp.float32)
    angles = jnp.arange(ANG).astype(jnp.float32) * (2.0 * math.pi / ANG)
    phase = orders[:, None] * angles[None, :]
    cosine = jnp.cos(phase)
    sine = jnp.sin(phase)
    upper = jnp.concatenate([cosine, sine], axis=1)
    lower = jnp.concatenate([-sine, cosine], axis=1)
    return (jnp.concatenate([upper, lower], axis=0) * (ORD ** -0.5)).astype(jnp.bfloat16)


def rotated_ops(tilts, azimuths, slice_ops):
    chosen = jnp.take(slice_ops, tilts, axis=0).astype(jnp.float32)
    chosen = jnp.transpose(chosen, (1, 0, 2))
    orders = (jnp.arange(LM) % ORD - ORD // 2).astype(jnp.float32)
    turns = azimuths.astype(jnp.float32) * (2.0 * math.pi / NAZI)
    phase = orders[:, None] * turns[None, :]
    cosine = jnp.cos(phase)[:, :, None]
    sine = jnp.sin(phase)[:, :, None]
    upper = jnp.concatenate([cosine * chosen, -sine * chosen], axis=2)
    lower = jnp.concatenate([sine * chosen, cosine * chosen], axis=2)
    rotator = jnp.concatenate([upper, lower], axis=0)
    return rotator.reshape(2 * LM, -1).astype(jnp.bfloat16)


def synthesize(coefs, rotator, angle_table):
    classes, radial = coefs.shape[0], coefs.shape[1]
    flat_coef = coefs.reshape(classes * radial, 2 * LM)
    harmonics = jnp.dot(flat_coef, rotator, preferred_element_type=jnp.float32).astype(jnp.bfloat16)
    orients = rotator.shape[1] // (2 * ORD)
    harmonics = harmonics.reshape(classes, radial, orients, 2 * ORD).transpose(2, 0, 1, 3).reshape(-1, 2 * ORD)
    values = jnp.dot(harmonics, angle_table, preferred_element_type=jnp.float32).astype(jnp.bfloat16)
    return values.reshape(orients * classes, radial * 2 * ANG)


def adjoint(back_proj, rotator, angle_table, radial, classes):
    columns = back_proj.shape[1]
    orients = rotator.shape[1] // (2 * ORD)
    spread = back_proj.reshape(radial, 2 * ANG, columns).transpose(0, 2, 1).reshape(radial * columns, 2 * ANG)
    harmonics = jnp.dot(spread, angle_table.T, preferred_element_type=jnp.float32).astype(jnp.bfloat16)
    harmonics = harmonics.reshape(radial, orients, classes, 2 * ORD).transpose(2, 0, 1, 3)
    harmonics = harmonics.reshape(classes * radial, orients * 2 * ORD)
    return lax.dot_general(harmonics, rotator, (((1,), (1,)), ((), ())), preferred_element_type=jnp.float32)


def reference(images, ctf_class, class_mask, precision, class_log_prior, ctf_filters, volume_coef, slice_ops, tilt_index, azimuth_index):
    angle_table = synth_table()
    ctf_rows = jnp.take(ctf_filters, ctf_class, axis=0)
    filtered = (images.astype(jnp.float32) * ctf_rows).astype(jnp.bfloat16)
    ctf_square = ctf_filters * ctf_filters
    tilt_blocks = tilt_index.reshape(N_ORI, ORI_DEV)
    azimuth_blocks = azimuth_index.reshape(N_ORI, ORI_DEV)

    def forward(block):
        rotator = rotated_ops(block[0], block[1], slice_ops)
        templates = synthesize(volume_coef, rotator, angle_table)
        correl = lax.dot_general(filtered, templates, (((1,), (1,)), ((), ())), preferred_element_type=jnp.float32)
        square = templates.astype(jnp.float32)
        square = square * square
        energy = lax.dot_general(ctf_square, square, (((1,), (1,)), ((), ())), precision=lax.Precision.HIGHEST)
        return correl, energy

    correl, energy = lax.map(forward, (tilt_blocks, azimuth_blocks))
    correl = correl.transpose(1, 0, 2).reshape(IMAGES, ORIENT * K)
    energy = energy.transpose(1, 0, 2).reshape(NCTF, ORIENT * K)
    energy_rows = jnp.take(energy, ctf_class, axis=0)
    score = precision[:, None] * (correl - 0.5 * energy_rows) + jnp.tile(class_log_prior, (1, ORIENT))
    allowed = jnp.tile(class_mask, (1, ORIENT)) > 0
    score = jnp.where(allowed, score, -1e30)
    row_peak = jnp.max(score, axis=1)
    exponent = jnp.exp(score - row_peak[:, None])
    totals = exponent.reshape(IMAGES, ORIENT, K).sum(axis=1)
    norm_sum = totals.sum(axis=1)
    log_evidence = row_peak + jnp.log(norm_sum)
    class_posterior = totals / norm_sum[:, None]
    weights = (exponent / norm_sum[:, None]).astype(jnp.bfloat16)
    back_proj = lax.dot_general(filtered, weights, (((0,), (0,)), ((), ())), preferred_element_type=jnp.float32)
    back_proj = back_proj.astype(jnp.bfloat16)
    back_blocks = back_proj.reshape(P_SIZE, N_ORI, ORI_DEV * K).transpose(1, 0, 2)

    def gather_coef(running, block):
        rotator = rotated_ops(block[0], block[1], slice_ops)
        return running + adjoint(block[2], rotator, angle_table, R, K), None

    initial = jnp.zeros((K * R, 2 * LM), jnp.float32)
    coef_sum, unused = lax.scan(gather_coef, initial, (tilt_blocks, azimuth_blocks, back_blocks))
    return coef_sum.reshape(K, R, 2, LM), log_evidence, class_posterior
```

```python
import functools
import math

import jax
import jax.numpy as jnp
import numpy as np
from jax import lax
from jax.experimental import pallas as pl
from jax.experimental.pallas import tpu as pltpu
from jax.sharding import PartitionSpec as P

ORD = 64
ANG = 128
NAZI = 32
HARM = 2 * ORD
RING = 2 * ANG
BIG = -1e30


F32 = jnp.float32
BF16 = jnp.bfloat16
VMEM = pl.BlockSpec(memory_space=pltpu.VMEM)
SMEM = pl.BlockSpec(memory_space=pltpu.SMEM)
NN = (((1,), (0,)), ((), ()))
NT = (((1,), (1,)), ((), ()))
TN = (((0,), (0,)), ((), ()))


def dot(a, b, dims=NN):
    return lax.dot_general(a, b, dims, preferred_element_type=F32)


def angle_table():
    orders = np.arange(ORD) - ORD // 2
    steps = (orders[:, None] * np.arange(ANG)[None, :]) % ANG
    phase = steps * (2.0 * math.pi / ANG)
    cosine, sine = np.cos(phase), np.sin(phase)
    table = np.concatenate(
        [np.concatenate([cosine, sine], 1), np.concatenate([-sine, cosine], 1)], 0
    )
    return jnp.asarray((table * ORD**-0.5).astype(np.float32)).astype(BF16)


def params(limit=48 << 20, **kw):
    return pltpu.CompilerParams(vmem_limit_bytes=limit, **kw)


def cost(flops, moved):
    return pl.CostEstimate(flops=int(flops), bytes_accessed=int(moved), transcendentals=0)


def split3(x):
    high = x.astype(BF16)
    rest = x - high.astype(F32)
    mid = rest.astype(BF16)
    low = (rest - mid.astype(F32)).astype(BF16)
    return high, mid, low


def harmonics_kernel(tilt_ref, azi_ref, coef_ref, ops_ref, out_ref, cos_ref, sin_ref, lhs_ref, acc_ref):
    step = pl.program_id(0)
    orients = azi_ref.shape[0]
    rows = coef_ref.shape[1]
    width = coef_ref.shape[2]
    lanes = cos_ref.shape[1]

    @pl.when(step == 0)
    def _():
        order = lax.broadcasted_iota(jnp.int32, (1, lanes), 1) & (NAZI - 1)
        turns = jnp.concatenate(
            [(order * azi_ref[o]) & (NAZI - 1) for o in range(orients)], axis=0
        )
        phase = turns.astype(F32) * (2.0 * math.pi / NAZI)
        cos_ref[...] = jnp.cos(phase)
        sin_ref[...] = jnp.sin(phase)
        acc_ref[...] = jnp.zeros_like(acc_ref)

    real = coef_ref[0].astype(F32)
    imag = coef_ref[1].astype(F32)
    for o in range(orients):
        c = jnp.tile(cos_ref[o : o + 1, :], (1, width // lanes))
        s = jnp.tile(sin_ref[o : o + 1, :], (1, width // lanes))
        base = o * 2 * rows
        lhs_ref[base : base + rows, :] = (c * real + s * imag).astype(BF16)
        lhs_ref[base + rows : base + 2 * rows, :] = (c * imag - s * real).astype(BF16)
    acc_ref[...] += dot(lhs_ref[...], ops_ref[...], NT)

    @pl.when(step == pl.num_programs(0) - 1)
    def _():
        left = lax.broadcasted_iota(jnp.int32, (rows, HARM), 1) < ORD
        shells = out_ref.shape[0]
        classes = rows // shells
        made = []
        for o in range(orients):
            tilt = tilt_ref[o]
            at = pl.multiple_of((tilt // 2) * HARM, HARM)
            odd = (tilt % 2) == 1
            base = o * 2 * rows
            re = acc_ref[base : base + rows, pl.ds(at, HARM)]
            im = acc_ref[base + rows : base + 2 * rows, pl.ds(at, HARM)]
            even_case = jnp.where(left, re, pltpu.roll(im, ORD, 1))
            odd_case = jnp.where(left, pltpu.roll(re, ORD, 1), im)
            made.append(jnp.where(odd, odd_case, even_case))
        for r in range(shells):
            for o in range(0, orients, 2):
                pair = jnp.concatenate(
                    [made[o][r * classes : (r + 1) * classes], made[o + 1][r * classes : (r + 1) * classes]], axis=0
                )
                out_ref[r, o * classes : (o + 2) * classes, :] = pair.astype(BF16)


def own_harmonics(tilts, azimuths, coefs, ops_t, shells, classes):
    orients = tilts.shape[0]
    rows = shells * classes
    total, length = ops_t.shape
    steps = 4
    width = length // steps
    return pl.pallas_call(
        harmonics_kernel,
        out_shape=jax.ShapeDtypeStruct((shells, orients * classes, HARM), BF16),
        grid=(steps,),
        in_specs=[
            SMEM,
            SMEM,
            pl.BlockSpec((2, rows, width), lambda j: (0, 0, j)),
            pl.BlockSpec((total, width), lambda j: (0, j)),
        ],
        out_specs=pl.BlockSpec((shells, orients * classes, HARM), lambda j: (0, 0, 0)),
        scratch_shapes=[
            pltpu.VMEM((orients, 128), F32),
            pltpu.VMEM((orients, 128), F32),
            pltpu.VMEM((orients * 2 * rows, width), BF16),
            pltpu.VMEM((orients * 2 * rows, total), F32),
        ],
        compiler_params=params(),
        cost_estimate=cost(2 * orients * 2 * rows * total * length, total * length * 2),
        name="harmonics",
    )(tilts, azimuths, coefs, ops_t)


def project_kernel(image_ref, class_ref, ctf_ref, table_ref, out_ref, parts_ref):
    filters = ctf_ref.shape[0]
    owners, _, per_owner = out_ref.shape

    @pl.when(pl.program_id(0) == 0)
    def _():
        for n, part in enumerate(split3(ctf_ref[...])):
            parts_ref[n * filters : (n + 1) * filters, :] = part

    index = class_ref[...]
    rows = index.shape[1]
    kind = lax.broadcasted_iota(jnp.int32, (filters, rows), 0)
    chosen = (kind == index).astype(F32)
    chosen = jnp.concatenate([chosen] * 3, axis=0).astype(BF16)
    table = table_ref[...]
    shells = per_owner // HARM
    for g in range(owners):
        for r in range(shells):
            at = (g * shells + r) * RING
            ctf = dot(chosen, parts_ref[:, at : at + RING], TN)
            kept = (image_ref[:, at : at + RING].astype(F32) * ctf).astype(BF16)
            out_ref[g, :, r * HARM : (r + 1) * HARM] = dot(kept, table, NT).astype(BF16)


def project_images(images, class_row, ctf, table, owners, shells):
    count, size = images.shape
    filters = ctf.shape[0]
    steps = 4
    block = count // steps
    return pl.pallas_call(
        project_kernel,
        out_shape=jax.ShapeDtypeStruct((owners, count, shells * HARM), BF16),
        grid=(steps,),
        in_specs=[
            pl.BlockSpec((block, size), lambda j: (j, 0)),
            pl.BlockSpec((1, block), lambda j: (0, j)),
            pl.BlockSpec((filters, size), lambda j: (0, 0)),
            pl.BlockSpec((HARM, RING), lambda j: (0, 0)),
        ],
        out_specs=pl.BlockSpec((owners, block, shells * HARM), lambda j: (0, j, 0)),
        scratch_shapes=[pltpu.VMEM((3 * filters, size), BF16)],
        compiler_params=params(),
        cost_estimate=cost(8 * count * size * 128, count * size * 3),
        name="project",
    )(images, class_row, ctf, table)


def score_kernel(owners, me_ref, *refs):
    pieces = refs[:owners]
    (proj_ref, ctf_ref, table_ref, class_ref, mask_ref, prec_ref, prior_ref, tilt_ref, azi_ref,
     exp_ref, stat_ref) = refs[owners:]
    me = me_ref[0]
    shells, cols, _ = pieces[0].shape
    filters = ctf_ref.shape[1]
    count = proj_ref.shape[1]
    classes = mask_ref.shape[0]
    table = table_ref[...]
    corr = jnp.zeros((cols, count), F32)
    energy = jnp.zeros((cols, 2 * filters), F32)
    for s in range(owners):
        block = me ^ s
        for r in range(shells):
            harm = pieces[s][r]
            corr += dot(harm, proj_ref[block, :, r * HARM : (r + 1) * HARM], NT)
            value = dot(harm, table).astype(BF16).astype(F32)
            square = value * value
            high = square.astype(BF16)
            low = (square - high.astype(F32)).astype(BF16)
            ctf = ctf_ref[block * shells + r]
            ctf = ctf * ctf
            ctf_high = ctf.astype(BF16)
            ctf_low = (ctf - ctf_high.astype(F32)).astype(BF16)
            both = jnp.concatenate([ctf_high, ctf_low], axis=0)
            energy += dot(high, both, NT) + dot(low, both, NT)
    energy = energy[:, :filters] + energy[:, filters:]
    kind = lax.broadcasted_iota(jnp.int32, (filters, count), 0)
    chosen = (kind == class_ref[...]).astype(F32).astype(BF16)
    rows = jnp.zeros((cols, count), F32)
    for part in split3(energy):
        rows += dot(part, chosen)
    tiles = cols // classes
    prior = prior_ref[...]
    allowed = mask_ref[...] > 0
    scale = prec_ref[...]
    made = scale * (corr - 0.5 * rows)
    made = made.reshape(tiles, classes, count) + prior[None]
    made = jnp.where(allowed[None], made, BIG)
    peak = jnp.max(jnp.max(made, axis=0), axis=0, keepdims=True)
    raised = jnp.exp(made - peak[None])
    exp_ref[...] = raised.reshape(cols, count)
    stat_ref[:classes, :] = jnp.sum(raised, axis=0)
    stat_ref[classes : classes + 1, :] = peak
    stat_ref[classes + 1 : classes + 2, :cols] = tilt_ref[...]
    stat_ref[classes + 1 : classes + 2, cols : 2 * cols] = azi_ref[...]
    stat_ref[classes + 1 : classes + 2, 2 * cols :] = jnp.zeros((1, count - 2 * cols), F32)
    stat_ref[classes + 2 :, :] = jnp.zeros((6, count), F32)


def local_scores(me, pieces, proj, ctf_blocks, table, class_row, mask_t, prec_row, prior_t, tilt_row, azi_row):
    owners = len(pieces)
    cols = pieces[0].shape[1]
    count = proj.shape[1]
    classes = mask_t.shape[0]
    return pl.pallas_call(
        functools.partial(score_kernel, owners),
        out_shape=(
            jax.ShapeDtypeStruct((cols, count), F32),
            jax.ShapeDtypeStruct((classes + 8, count), F32),
        ),
        in_specs=[SMEM] + [VMEM] * (owners + 9),
        out_specs=(VMEM, VMEM),
        compiler_params=params(),
        cost_estimate=cost(4 * cols * count * owners * proj.shape[2], proj.size * 2),
        name="score",
    )(me, *pieces, proj, ctf_blocks, table, class_row, mask_t, prec_row, prior_t, tilt_row, azi_row)


def back_kernel(parts, me_ref, *refs):
    stats = refs[:parts]
    exp_ref, proj_ref, keep_ref, send_ref, evid_ref, post_ref = refs[parts:]
    me = me_ref[0]
    owners, count, per_owner = proj_ref.shape
    classes = post_ref.shape[0]
    shells = per_owner // HARM
    peaks = [s[classes : classes + 1, :] for s in stats]
    top = functools.reduce(jnp.maximum, peaks)
    totals = jnp.zeros((classes, count), F32)
    for s, p in zip(stats, peaks):
        totals += s[:classes, :] * jnp.exp(p - top)
    norm = jnp.sum(totals, axis=0, keepdims=True)
    evid_ref[...] = top + jnp.log(norm)
    post_ref[...] = totals / norm
    weights = (exp_ref[...] * (jnp.exp(peaks[0] - top) / norm)).astype(BF16)
    for s in range(owners):
        made = dot(weights, proj_ref[me ^ s]).astype(BF16)
        target = send_ref if s % 2 else keep_ref
        for r in range(shells):
            target[s // 2, r] = made[:, r * HARM : (r + 1) * HARM]


def back_project(me, stats, raised, proj, classes):
    cols, count = raised.shape
    owners, _, per_owner = proj.shape
    shells = per_owner // HARM
    half = jax.ShapeDtypeStruct((owners // 2, shells, cols, HARM), BF16)
    return pl.pallas_call(
        functools.partial(back_kernel, len(stats)),
        out_shape=(
            half,
            half,
            jax.ShapeDtypeStruct((1, count), F32),
            jax.ShapeDtypeStruct((classes, count), F32),
        ),
        in_specs=[SMEM] + [VMEM] * (len(stats) + 2),
        out_specs=(VMEM,) * 4,
        compiler_params=params(),
        cost_estimate=cost(2 * cols * count * owners * per_owner, proj.size * 2),
        name="back",
    )(me, *stats, raised, proj)


def phase_kernel(classes, cols, *refs):
    *stats, weight_ref, tilt_ref = refs
    info = [s[classes + 1 : classes + 2, :] for s in stats]
    total = len(stats) * cols
    azimuth = jnp.concatenate([i[:, cols : 2 * cols] for i in info], axis=1).astype(jnp.int32)
    for n, i in enumerate(info):
        tilt_ref[n * cols : (n + 1) * cols, :] = jnp.transpose(jnp.broadcast_to(i[:, :cols], (cols, cols)))
    order = lax.broadcasted_iota(jnp.int32, (NAZI, total), 0)
    phase = ((order * azimuth) & (NAZI - 1)).astype(F32) * (2.0 * math.pi / NAZI)
    cosine, sine = jnp.cos(phase), jnp.sin(phase)
    row = lax.broadcasted_iota(jnp.int32, (classes, total), 0)
    lane = lax.broadcasted_iota(jnp.int32, (classes, total), 1) % classes
    same = row == lane
    for n in range(NAZI):
        c = jnp.where(same, cosine[n : n + 1], 0.0)
        s = jnp.where(same, sine[n : n + 1], 0.0)
        at = n * 2 * classes
        weight_ref[at : at + 2 * classes, :total] = jnp.concatenate([c, s], axis=0).astype(BF16)
        weight_ref[at : at + 2 * classes, total:] = jnp.concatenate([-s, c], axis=0).astype(BF16)


def all_phases(stats, classes, cols):
    total = len(stats) * cols
    return pl.pallas_call(
        functools.partial(phase_kernel, classes, cols),
        out_shape=(
            jax.ShapeDtypeStruct((NAZI * 2 * classes, 2 * total), BF16),
            jax.ShapeDtypeStruct((total, cols), F32),
        ),
        in_specs=[VMEM] * len(stats),
        out_specs=(VMEM, VMEM),
        compiler_params=params(),
        cost_estimate=cost(2e8, 4e6),
        name="phases",
    )(*stats)


def coef_kernel(parts, *refs):
    pieces = refs[:parts]
    weight_ref, tilt_ref, ops_ref, out_ref, spread_ref, rows_ref = refs[parts:]
    shells, cols, _ = pieces[0].shape
    total = ops_ref.shape[0]
    width = ops_ref.shape[1]
    groups = weight_ref.shape[0]

    @pl.when(pl.program_id(0) == 0)
    def _():
        left = lax.broadcasted_iota(jnp.int32, (cols, HARM), 1) < ORD
        block = lax.broadcasted_iota(jnp.int32, (cols, HARM), 1) // ORD
        for r in range(shells):
            for n in range(parts):
                value = pieces[n][r].astype(F32)
                turned = pltpu.roll(value, ORD, 1)
                real = jnp.where(left, value, turned)
                imag = jnp.where(left, turned, value)
                tilt = tilt_ref[n * cols : (n + 1) * cols, :HARM].astype(jnp.int32)
                for b in range(total // HARM):
                    mine = tilt == block + 2 * b
                    at = slice(b * HARM, (b + 1) * HARM)
                    spread_ref[n * cols : (n + 1) * cols, at] = jnp.where(mine, real, 0.0).astype(BF16)
                    spread_ref[(parts + n) * cols : (parts + n + 1) * cols, at] = jnp.where(
                        mine, imag, 0.0
                    ).astype(BF16)
            rows_ref[r] = dot(weight_ref[...], spread_ref[...]).astype(BF16)

    lane = lax.broadcasted_iota(jnp.int32, (groups // NAZI, width), 1) & (NAZI - 1)
    for r in range(shells):
        made = dot(rows_ref[r], ops_ref[...]).reshape(NAZI, groups // NAZI, width)
        out = made[0]
        for n in range(1, NAZI):
            out = jnp.where(lane == n, made[n], out)
        out_ref[r] = out


def final_coefs(pieces, weights, tilts, ops_t, classes):
    parts = len(pieces)
    shells, cols, _ = pieces[0].shape
    total, length = ops_t.shape
    groups = weights.shape[0]
    steps = 8
    width = length // steps
    full = lambda a: pl.BlockSpec(a.shape, lambda j: (0,) * a.ndim)
    return pl.pallas_call(
        functools.partial(coef_kernel, parts),
        out_shape=jax.ShapeDtypeStruct((shells, 2 * classes, length), F32),
        grid=(steps,),
        in_specs=[full(p) for p in pieces]
        + [full(weights), full(tilts), pl.BlockSpec((total, width), lambda j: (0, j))],
        out_specs=pl.BlockSpec((shells, 2 * classes, width), lambda j: (0, 0, j)),
        scratch_shapes=[
            pltpu.VMEM((2 * parts * cols, total), BF16),
            pltpu.VMEM((shells, groups, total), BF16),
        ],
        compiler_params=params(),
        cost_estimate=cost(2 * shells * groups * total * length, total * length * 2),
        name="coefs",
    )(*pieces, weights, tilts, ops_t)


def swap(x, axis, size, offset):
    return lax.ppermute(x, axis, [(i, i ^ offset) for i in range(size)])


def body(
    n_img,
    n_ori,
    images,
    ctf_class,
    class_mask,
    precision,
    class_log_prior,
    ctf_filters,
    volume_coef,
    slice_ops,
    tilt_index,
    azimuth_index,
):
    classes, shells, _, length = volume_coef.shape
    orients = tilt_index.shape[0]
    count, size = images.shape
    cols = orients * classes
    table = angle_table()
    me = lax.axis_index("img").astype(jnp.int32).reshape(1)
    class_row = ctf_class.reshape(1, count)
    ops_t = jnp.transpose(slice_ops, (0, 2, 1)).reshape(-1, length)
    coefs = jnp.transpose(volume_coef, (2, 1, 0, 3)).reshape(2, shells * classes, length)

    own = own_harmonics(tilt_index, azimuth_index, coefs, ops_t, shells, classes)
    even = [own] + [swap(own, "img", n_img, s) for s in range(2, n_img, 2)]
    odd = [swap(p, "img", n_img, 1) for p in even]
    pieces = [p for pair in zip(even, odd) for p in pair]

    proj = project_images(images, class_row, ctf_filters, table, n_img, shells)

    ctf_blocks = jnp.transpose(ctf_filters.reshape(-1, size // RING, RING), (1, 0, 2))
    tilt_row = jnp.repeat(tilt_index.astype(F32), classes).reshape(1, cols)
    azi_row = jnp.repeat(azimuth_index.astype(F32), classes).reshape(1, cols)
    raised, stat = local_scores(
        me,
        pieces,
        proj,
        ctf_blocks,
        table,
        class_row,
        class_mask.T,
        precision.reshape(1, count),
        class_log_prior.T,
        tilt_row,
        azi_row,
    )
    stats = [stat] + [swap(stat, "ori", n_ori, s) for s in range(1, n_ori)]
    keep, send, evidence, posterior = back_project(me, stats, raised, proj, classes)
    came = swap(send, "img", n_img, 1)
    chip = (keep.astype(F32) + came.astype(F32)).astype(BF16)
    weights, tilts = all_phases(stats, classes, cols)
    mine = chip[0].astype(F32)
    for s in range(2, n_img, 2):
        mine = mine + swap(chip[s // 2], "img", n_img, s).astype(F32)
    mine = mine.astype(BF16)
    sums = [mine] + [swap(mine, "ori", n_ori, s) for s in range(1, n_ori)]
    coef = final_coefs(sums, weights, tilts, ops_t, classes)
    coef = coef.reshape(shells, 2, classes, length).transpose(2, 0, 1, 3)
    return coef, evidence.reshape(count), posterior.T


def solution(mesh):
    placed = (
        P("img", None),
        P("img"),
        P("img", None),
        P("img"),
        P("img", None),
        P(),
        P(None, "img", None, None),
        P(),
        P("ori"),
        P("ori"),
    )
    return jax.shard_map(
        functools.partial(body, mesh.shape["img"], mesh.shape["ori"]),
        mesh=mesh,
        in_specs=placed,
        out_specs=(P(None, "img", None, None), P("img"), P("img", None)),
        check_vma=False,
    )
```

```python
import functools
import math

import jax
import jax.numpy as jnp
import numpy as np
from jax import lax
from jax.experimental import pallas as pl
from jax.experimental.pallas import tpu as pltpu
from jax.sharding import PartitionSpec as P

ORD = 64
ANG = 128
NAZI = 32
HARM = 2 * ORD
RING = 2 * ANG
BIG = -1e30


F32 = jnp.float32
BF16 = jnp.bfloat16
VMEM = pl.BlockSpec(memory_space=pltpu.VMEM)
SMEM = pl.BlockSpec(memory_space=pltpu.SMEM)
HBM = pl.BlockSpec(memory_space=pltpu.HBM)
NN = (((1,), (0,)), ((), ()))
NT = (((1,), (1,)), ((), ()))
TN = (((0,), (0,)), ((), ()))


def dot(a, b, dims=NN):
    return lax.dot_general(a, b, dims, preferred_element_type=F32)


def angle_table():
    orders = np.arange(ORD) - ORD // 2
    steps = (orders[:, None] * np.arange(ANG)[None, :]) % ANG
    phase = steps * (2.0 * math.pi / ANG)
    cosine, sine = np.cos(phase), np.sin(phase)
    table = np.concatenate(
        [np.concatenate([cosine, sine], 1), np.concatenate([-sine, cosine], 1)], 0
    )
    return jnp.asarray((table * ORD**-0.5).astype(np.float32)).astype(BF16)


def params(limit=48 << 20, **kw):
    return pltpu.CompilerParams(vmem_limit_bytes=limit, **kw)


def cost(flops, moved):
    return pl.CostEstimate(flops=int(flops), bytes_accessed=int(moved), transcendentals=0)


def split3(x):
    high = x.astype(BF16)
    rest = x - high.astype(F32)
    mid = rest.astype(BF16)
    low = (rest - mid.astype(F32)).astype(BF16)
    return high, mid, low


def column(row, size):
    lanes = row.shape[1]
    here = lax.broadcasted_iota(jnp.int32, (size, lanes), 1) == lax.broadcasted_iota(jnp.int32, (size, lanes), 0)
    return jnp.sum(jnp.where(here, jnp.broadcast_to(row, (size, lanes)), 0.0), axis=1, keepdims=True)


def harmonics_kernel(tilt_hbm, azi_hbm, coef_hbm, ops_hbm, out_ref, tilt_ref, azi_ref, coef_ref, ops_ref, lhs_ref, acc_ref, sem):
    classes, shells, _, length = coef_ref.shape
    orients = tilt_ref.shape[1]
    total = ops_ref.shape[0]
    steps = ops_sem_count(sem)
    width = length // steps
    pairs = classes * shells
    copies = [
        pltpu.make_async_copy(azi_hbm, azi_ref, sem.at[steps]),
        pltpu.make_async_copy(tilt_hbm, tilt_ref, sem.at[steps + 1]),
        pltpu.make_async_copy(coef_hbm, coef_ref, sem.at[steps + 2]),
    ]
    blocks = []
    for n in range(steps):
        at = pl.ds(n * width, width)
        blocks.append(pltpu.make_async_copy(ops_hbm.at[:, at], ops_ref.at[:, at], sem.at[n]))
    for copy in copies + blocks:
        copy.start()
    copies[0].wait()
    copies[1].wait()
    turn = column(azi_ref[...].astype(F32), orients).astype(jnp.int32)
    order = lax.broadcasted_iota(jnp.int32, (orients, 128), 1) & (NAZI - 1)
    phase = ((order * turn) & (NAZI - 1)).astype(F32) * (2.0 * math.pi / NAZI)
    cosine, sine = jnp.cos(phase), jnp.sin(phase)
    copies[2].wait()
    for n in range(steps):
        for r in range(shells):
            for k in range(classes):
                base = (r * classes + k) * orients
                for j in range(width // 128):
                    at = n * width + j * 128
                    both = coef_ref[k, r, :, at : at + 128].astype(F32)
                    real = jnp.broadcast_to(both[0:1], (orients, 128))
                    imag = jnp.broadcast_to(both[1:2], (orients, 128))
                    lanes = slice(j * 128, (j + 1) * 128)
                    lhs_ref[n % 2, base : base + orients, lanes] = (cosine * real + sine * imag).astype(BF16)
                    lhs_ref[n % 2, (pairs * orients) + base : (pairs * orients) + base + orients, lanes] = (
                        cosine * imag - sine * real
                    ).astype(BF16)
        blocks[n].wait()
        part = dot(lhs_ref[n % 2], ops_ref[:, n * width : (n + 1) * width], NT)
        if n == 0:
            acc_ref[...] = part
        else:
            acc_ref[...] += part
    tilt = column(tilt_ref[...].astype(F32), orients)
    left = lax.broadcasted_iota(jnp.int32, (orients, HARM), 1) < ORD
    odd = jnp.zeros((orients, 1), jnp.bool_)
    for b in range(1, total // ORD, 2):
        odd = odd | (tilt == float(b))
    for r in range(shells):
        for k in range(classes):
            base = (r * classes + k) * orients
            chosen = []
            for half in range(2):
                top = half * pairs * orients + base
                value = acc_ref[top : top + orients, 0:HARM]
                for j in range(1, total // HARM):
                    mine = (tilt >= 2.0 * j) & (tilt < 2.0 * j + 2.0)
                    value = jnp.where(mine, acc_ref[top : top + orients, j * HARM : (j + 1) * HARM], value)
                chosen.append(value)
            re, im = chosen
            even_case = jnp.where(left, re, pltpu.roll(im, ORD, 1))
            odd_case = jnp.where(left, pltpu.roll(re, ORD, 1), im)
            out_ref[r, k * orients : (k + 1) * orients, :] = jnp.where(odd, odd_case, even_case).astype(BF16)


def ops_sem_count(sem):
    return sem.shape[0] - 3


def own_harmonics(tilts, azimuths, coefs, ops_t):
    classes, shells, _, length = coefs.shape
    orients = tilts.shape[1]
    total = ops_t.shape[0]
    steps = 4
    rows = 2 * classes * shells * orients
    return pl.pallas_call(
        harmonics_kernel,
        out_shape=jax.ShapeDtypeStruct((shells, orients * classes, HARM), BF16),
        in_specs=[HBM] * 4,
        out_specs=VMEM,
        scratch_shapes=[
            pltpu.VMEM(tilts.shape, jnp.int32),
            pltpu.VMEM(azimuths.shape, jnp.int32),
            pltpu.VMEM(coefs.shape, BF16),
            pltpu.VMEM(ops_t.shape, BF16),
            pltpu.VMEM((2, rows, length // steps), BF16),
            pltpu.VMEM((rows, total), F32),
            pltpu.SemaphoreType.DMA((steps + 3,)),
        ],
        compiler_params=params(),
        cost_estimate=cost(2 * rows * total * length, total * length * 2),
        name="harmonics",
    )(tilts, azimuths, coefs, ops_t)


def project_kernel(image_ref, class_ref, ctf_ref, table_ref, out_ref):
    filters = ctf_ref.shape[0]
    owners, count, per_owner = out_ref.shape
    kind = lax.broadcasted_iota(jnp.int32, (filters, count), 0)
    chosen = (kind == class_ref[...]).astype(F32)
    chosen = jnp.transpose(jnp.concatenate([chosen] * 3, axis=0)).astype(BF16)
    table = table_ref[...]
    shells = per_owner // HARM
    for g in range(owners):
        for r in range(shells):
            at = (g * shells + r) * RING
            parts = jnp.concatenate(split3(ctf_ref[:, at : at + RING]), axis=0)
            kept = (image_ref[:, at : at + RING].astype(F32) * dot(chosen, parts)).astype(BF16)
            out_ref[g, :, r * HARM : (r + 1) * HARM] = dot(kept, table, NT).astype(BF16)


def project_images(images, class_row, ctf, table, owners, shells):
    count, size = images.shape
    return pl.pallas_call(
        project_kernel,
        out_shape=jax.ShapeDtypeStruct((owners, count, shells * HARM), BF16),
        in_specs=[VMEM] * 4,
        out_specs=VMEM,
        compiler_params=params(),
        cost_estimate=cost(8 * count * size * 128, count * size * 3),
        name="project",
    )(images, class_row, ctf, table)


def score_kernel(owners, me_ref, *refs):
    pieces = refs[:owners]
    (proj_ref, ctf_ref, table_ref, class_ref, mask_ref, prec_ref, prior_ref, tilt_ref, azi_ref,
     exp_ref, stat_ref) = refs[owners:]
    me = me_ref[0]
    shells, cols, _ = pieces[0].shape
    filters = ctf_ref.shape[1]
    count = proj_ref.shape[1]
    classes = mask_ref.shape[0]
    orients = cols // classes
    table = table_ref[...]
    corr = jnp.zeros((cols, count), F32)
    energy = jnp.zeros((cols, 2 * filters), F32)
    for s in range(owners):
        block = me ^ s
        harm = [pieces[s][r] for r in range(shells)]
        corr += dot(jnp.concatenate(harm, axis=1), proj_ref[block], NT)
        for r in range(shells):
            value = dot(harm[r], table).astype(BF16).astype(F32)
            square = value * value
            high = square.astype(BF16)
            low = (square - high.astype(F32)).astype(BF16)
            ctf = ctf_ref[block * shells + r]
            ctf = ctf * ctf
            ctf_high = ctf.astype(BF16)
            ctf_low = (ctf - ctf_high.astype(F32)).astype(BF16)
            both = jnp.concatenate([ctf_high, ctf_low], axis=0)
            energy += dot(high, both, NT) + dot(low, both, NT)
    energy = energy[:, :filters] + energy[:, filters:]
    kind = lax.broadcasted_iota(jnp.int32, (filters, count), 0)
    chosen = (kind == class_ref[...]).astype(F32).astype(BF16)
    rows = jnp.zeros((cols, count), F32)
    for part in split3(energy):
        rows += dot(part, chosen)
    made = prec_ref[...] * (corr - 0.5 * rows)
    peak = None
    scores = []
    for k in range(classes):
        score = made[k * orients : (k + 1) * orients] + prior_ref[k : k + 1, :]
        score = jnp.where(mask_ref[k : k + 1, :] > 0, score, BIG)
        scores.append(score)
        high = jnp.max(score, axis=0, keepdims=True)
        peak = high if peak is None else jnp.maximum(peak, high)
    for k in range(classes):
        raised = jnp.exp(scores[k] - peak)
        exp_ref[k * orients : (k + 1) * orients, :] = raised
        stat_ref[k : k + 1, :] = jnp.sum(raised, axis=0, keepdims=True)
    stat_ref[classes : classes + 1, :] = peak
    spread = lax.broadcasted_iota(jnp.int32, (orients, count), 0) == (
        lax.broadcasted_iota(jnp.int32, (orients, count), 1) % orients
    )
    for n, ref in enumerate((tilt_ref, azi_ref)):
        line = jnp.broadcast_to(ref[...].astype(F32), (8, orients)).astype(BF16)
        line = dot(line, spread.astype(F32).astype(BF16))
        stat_ref[classes + 1 + n : classes + 2 + n, :] = line[0:1]
    stat_ref[classes + 3 :, :] = jnp.zeros((5, count), F32)


def local_scores(me, pieces, proj, ctf_blocks, table, class_row, mask_t, prec_row, prior_t, tilt_row, azi_row):
    owners = len(pieces)
    cols = pieces[0].shape[1]
    count = proj.shape[1]
    classes = mask_t.shape[0]
    return pl.pallas_call(
        functools.partial(score_kernel, owners),
        out_shape=(
            jax.ShapeDtypeStruct((cols, count), F32),
            jax.ShapeDtypeStruct((classes + 8, count), F32),
        ),
        in_specs=[SMEM] + [VMEM] * (owners + 9),
        out_specs=(VMEM, VMEM),
        compiler_params=params(),
        cost_estimate=cost(4 * cols * count * owners * proj.shape[2], proj.size * 2),
        name="score",
    )(me, *pieces, proj, ctf_blocks, table, class_row, mask_t, prec_row, prior_t, tilt_row, azi_row)


def back_kernel(parts, me_ref, *refs):
    stats = refs[:parts]
    exp_ref, proj_ref, keep_ref, send_ref, evid_ref, post_ref = refs[parts:]
    me = me_ref[0]
    owners, count, per_owner = proj_ref.shape
    classes = post_ref.shape[0]
    shells = per_owner // HARM
    peaks = [s[classes : classes + 1, :] for s in stats]
    top = functools.reduce(jnp.maximum, peaks)
    totals = jnp.zeros((classes, count), F32)
    for s, p in zip(stats, peaks):
        totals += s[:classes, :] * jnp.exp(p - top)
    norm = jnp.sum(totals, axis=0, keepdims=True)
    evid_ref[...] = top + jnp.log(norm)
    post_ref[...] = totals / norm
    weights = (exp_ref[...] * (jnp.exp(peaks[0] - top) / norm)).astype(BF16)
    for s in range(owners):
        made = dot(weights, proj_ref[me ^ s]).astype(BF16)
        target = send_ref if s % 2 else keep_ref
        for r in range(shells):
            target[s // 2, r] = made[:, r * HARM : (r + 1) * HARM]


def back_project(me, stats, raised, proj, classes):
    cols, count = raised.shape
    owners, _, per_owner = proj.shape
    shells = per_owner // HARM
    half = jax.ShapeDtypeStruct((owners // 2, shells, cols, HARM), BF16)
    return pl.pallas_call(
        functools.partial(back_kernel, len(stats)),
        out_shape=(
            half,
            half,
            jax.ShapeDtypeStruct((1, count), F32),
            jax.ShapeDtypeStruct((classes, count), F32),
        ),
        in_specs=[SMEM] + [VMEM] * (len(stats) + 2),
        out_specs=(VMEM,) * 4,
        compiler_params=params(),
        cost_estimate=cost(2 * cols * count * owners * per_owner, proj.size * 2),
        name="back",
    )(me, *stats, raised, proj)


def phase_kernel(classes, cols, *refs):
    *stats, weight_ref, tilt_ref = refs
    total = len(stats) * cols
    azimuth = jnp.concatenate([s[classes + 2 : classes + 3, :cols] for s in stats], axis=1).astype(jnp.int32)
    for n, s in enumerate(stats):
        line = s[classes + 1 : classes + 2, :cols]
        tilt_ref[n * cols : (n + 1) * cols, :] = jnp.transpose(jnp.broadcast_to(line, (cols, cols)))
    order = lax.broadcasted_iota(jnp.int32, (NAZI, total), 0)
    phase = ((order * azimuth) & (NAZI - 1)).astype(F32) * (2.0 * math.pi / NAZI)
    cosine, sine = jnp.cos(phase), jnp.sin(phase)
    row = lax.broadcasted_iota(jnp.int32, (classes, total), 0)
    lane = (lax.broadcasted_iota(jnp.int32, (classes, total), 1) % cols) // (cols // classes)
    same = row == lane
    for n in range(NAZI):
        c = jnp.where(same, cosine[n : n + 1], 0.0)
        s = jnp.where(same, sine[n : n + 1], 0.0)
        at = n * 2 * classes
        weight_ref[at : at + 2 * classes, :total] = jnp.concatenate([c, s], axis=0).astype(BF16)
        weight_ref[at : at + 2 * classes, total:] = jnp.concatenate([-s, c], axis=0).astype(BF16)


def all_phases(stats, classes, cols):
    total = len(stats) * cols
    return pl.pallas_call(
        functools.partial(phase_kernel, classes, cols),
        out_shape=(
            jax.ShapeDtypeStruct((NAZI * 2 * classes, 2 * total), BF16),
            jax.ShapeDtypeStruct((total, cols), F32),
        ),
        in_specs=[VMEM] * len(stats),
        out_specs=(VMEM, VMEM),
        compiler_params=params(),
        cost_estimate=cost(2e8, 4e6),
        name="phases",
    )(*stats)


def coef_kernel(parts, *refs):
    pieces = refs[:parts]
    weight_ref, tilt_ref, ops_ref, out_hbm, spread_ref, rows_ref, made_ref, sem = refs[parts:]
    shells, cols, _ = pieces[0].shape
    total, length = ops_ref.shape
    groups = weight_ref.shape[0]
    classes = groups // NAZI // 2
    steps = sem.shape[0]
    width = length // steps
    left = lax.broadcasted_iota(jnp.int32, (cols, HARM), 1) < ORD
    block = lax.broadcasted_iota(jnp.int32, (cols, HARM), 1) // ORD
    for r in range(shells):
        for n in range(parts):
            value = pieces[n][r].astype(F32)
            turned = pltpu.roll(value, ORD, 1)
            real = jnp.where(left, value, turned)
            imag = jnp.where(left, turned, value)
            tilt = tilt_ref[n * cols : (n + 1) * cols, :HARM].astype(jnp.int32)
            for b in range(total // HARM):
                mine = tilt == block + 2 * b
                at = slice(b * HARM, (b + 1) * HARM)
                spread_ref[n * cols : (n + 1) * cols, at] = jnp.where(mine, real, 0.0).astype(BF16)
                spread_ref[(parts + n) * cols : (parts + n + 1) * cols, at] = jnp.where(mine, imag, 0.0).astype(BF16)
        rows_ref[r] = dot(weight_ref[...], spread_ref[...]).astype(BF16)
    lane = lax.broadcasted_iota(jnp.int32, (2 * classes, width), 1) & (NAZI - 1)
    copies = []
    for j in range(steps):
        at = slice(j * width, (j + 1) * width)
        for r in range(shells):
            made = dot(rows_ref[r], ops_ref[:, at]).reshape(NAZI, 2 * classes, width)
            out = made[0]
            for n in range(1, NAZI):
                out = jnp.where(lane == n, made[n], out)
            for half in range(2):
                made_ref[:, r, half, at] = out[half * classes : (half + 1) * classes]
        copy = pltpu.make_async_copy(made_ref.at[:, :, :, pl.ds(j * width, width)], out_hbm.at[:, :, :, pl.ds(j * width, width)], sem.at[j])
        copy.start()
        copies.append(copy)
    for copy in copies:
        copy.wait()


def final_coefs(pieces, weights, tilts, ops_t, classes):
    parts = len(pieces)
    shells, cols, _ = pieces[0].shape
    total, length = ops_t.shape
    groups = weights.shape[0]
    steps = 8
    return pl.pallas_call(
        functools.partial(coef_kernel, parts),
        out_shape=jax.ShapeDtypeStruct((classes, shells, 2, length), F32),
        in_specs=[VMEM] * (parts + 3),
        out_specs=HBM,
        scratch_shapes=[
            pltpu.VMEM((2 * parts * cols, total), BF16),
            pltpu.VMEM((shells, groups, total), BF16),
            pltpu.VMEM((classes, shells, 2, length), F32),
            pltpu.SemaphoreType.DMA((steps,)),
        ],
        compiler_params=params(),
        cost_estimate=cost(2 * shells * groups * total * length, total * length * 2),
        name="coefs",
    )(*pieces, weights, tilts, ops_t)


def swap(x, axis, size, offset):
    return lax.ppermute(x, axis, [(i, i ^ offset) for i in range(size)])


def body(
    n_img,
    n_ori,
    images,
    ctf_class,
    class_mask,
    precision,
    class_log_prior,
    ctf_filters,
    volume_coef,
    slice_ops,
    tilt_index,
    azimuth_index,
):
    classes, shells, _, length = volume_coef.shape
    orients = tilt_index.shape[0]
    count, size = images.shape
    cols = orients * classes
    table = angle_table()
    me = lax.axis_index("img").astype(jnp.int32).reshape(1)
    class_row = ctf_class.reshape(1, count)
    ops_t = jnp.transpose(slice_ops, (0, 2, 1)).reshape(-1, length)
    tilt_row = tilt_index.reshape(1, orients)
    azi_row = azimuth_index.reshape(1, orients)

    own = own_harmonics(tilt_row, azi_row, volume_coef, ops_t)
    proj = project_images(images, class_row, ctf_filters, table, n_img, shells)
    even = [own] + [swap(own, "img", n_img, s) for s in range(2, n_img, 2)]
    *even, proj = lax.optimization_barrier((*even, proj))
    odd = [swap(p, "img", n_img, 1) for p in even]
    pieces = [p for pair in zip(even, odd) for p in pair]

    ctf_blocks = jnp.transpose(ctf_filters.reshape(-1, size // RING, RING), (1, 0, 2))
    raised, stat = local_scores(
        me,
        pieces,
        proj,
        ctf_blocks,
        table,
        class_row,
        class_mask.T,
        precision.reshape(1, count),
        class_log_prior.T,
        tilt_row,
        azi_row,
    )
    stats = [stat] + [swap(stat, "ori", n_ori, s) for s in range(1, n_ori)]
    keep, send, evidence, posterior = back_project(me, stats, raised, proj, classes)
    came = swap(send, "img", n_img, 1)
    chip = (keep.astype(F32) + came.astype(F32)).astype(BF16)
    weights, tilts = all_phases(stats, classes, cols)
    mine = chip[0].astype(F32)
    for s in range(2, n_img, 2):
        mine = mine + swap(chip[s // 2], "img", n_img, s).astype(F32)
    mine = mine.astype(BF16)
    sums = [mine] + [swap(mine, "ori", n_ori, s) for s in range(1, n_ori)]
    coef = final_coefs(sums, weights, tilts, ops_t, classes)
    return coef, evidence.reshape(count), posterior.T


def solution(mesh):
    placed = (
        P("img", None),
        P("img"),
        P("img", None),
        P("img"),
        P("img", None),
        P(),
        P(None, "img", None, None),
        P(),
        P("ori"),
        P("ori"),
    )
    return jax.shard_map(
        functools.partial(body, mesh.shape["img"], mesh.shape["ori"]),
        mesh=mesh,
        in_specs=placed,
        out_specs=(P(None, "img", None, None), P("img"), P("img", None)),
        check_vma=False,
    )
```
